128 devices in a mesh: dp: 1, tp: 2 (over core), cp: 64 (over z, y, x).
Axes of the slice: x: 4, y: 4, z: 4, core: 2. Of those that a mesh axis runs over, the one named last changes fastest.
Arguments:
- x: bfloat16 [16384, 4096], P(('dp', 'cp'))
- k_cache: bfloat16 [16384, 2, 128], P(('dp', 'cp'), 'tp')
- v_cache: bfloat16 [16384, 2, 128], P(('dp', 'cp'), 'tp')
- rope_table: float32 [16384, 64], P(('dp', 'cp'))
- norm_gain: bfloat16 [4096], replicated
- w_qkv: bfloat16 [4096, 4608], P(None, 'tp')
- b_qkv: bfloat16 [4608], P('tp')
- w_out: bfloat16 [4096, 4096], P('tp')
Outputs:
- output 1: bfloat16 [16384, 4096], P(('dp', 'cp'))
- output 2: bfloat16 [16384, 2, 128], P(('dp', 'cp'), 'tp')
- output 3: bfloat16 [16384, 2, 128], P(('dp', 'cp'), 'tp')
All inputs are finite; a program needn't handle non-finite values.
Results may differ from the reference program's by a relative error of at most 0.00350049.
Values are sent between devices in bfloat16 or wider.
A program may use at most 1 GiB of HBM per device.

```python
import math
import jax
import jax.numpy as jnp
from jax import lax

D = 4096
HEADS = 32
KV_HEADS = 2
HEAD = 128
NEW_TOKENS = 16384
PREFIX = 16384
EPS = 1.5625e-07
MASK_VALUE = -1e30
GROUP = HEADS // KV_HEADS
QKV_WIDTH = (HEADS + 2 * KV_HEADS) * HEAD
PAIR_COUNT = HEAD // 4
QUERY_BLOCK = math.gcd(NEW_TOKENS, 128)
KEY_BLOCK = math.gcd(PREFIX + NEW_TOKENS, 512)


def setup_inputs(seed: int = 0, part: int = 0) -> dict:
    part_keys = jax.random.split(jax.random.fold_in(jax.random.key(seed), part), 4)
    shared_keys = jax.random.split(jax.random.key(seed + 1), 4)
    x = jax.random.normal(part_keys[0], (NEW_TOKENS, D), jnp.float32)
    k_cache = 1.6 * jax.random.normal(part_keys[1], (PREFIX, KV_HEADS, HEAD), jnp.float32)
    v_cache = 1.6 * jax.random.normal(part_keys[2], (PREFIX, KV_HEADS, HEAD), jnp.float32)
    log_ratio = jax.random.uniform(part_keys[3], (), jnp.float32, math.log(100.0), math.log(10000.0))
    rope_base = 10000.0 * jnp.exp(log_ratio)
    inv_freq = rope_base ** (-jnp.arange(PAIR_COUNT, dtype=jnp.float32) / PAIR_COUNT)
    positions = (PREFIX + jnp.arange(NEW_TOKENS)).astype(jnp.float32)
    angles = positions[:, None] * inv_freq[None, :]
    rope_table = jnp.concatenate([jnp.cos(angles), jnp.sin(angles)], axis=1)
    norm_gain = 1.0 + 0.3 * jax.random.normal(shared_keys[0], (D,), jnp.float32)
    w_qkv = jax.random.normal(shared_keys[1], (D, QKV_WIDTH), jnp.float32) * (1.5 / math.sqrt(D))
    b_qkv = 0.5 * jax.random.normal(shared_keys[2], (QKV_WIDTH,), jnp.float32)
    w_out = jax.random.normal(shared_keys[3], (HEADS * HEAD, D), jnp.float32) / math.sqrt(HEADS * HEAD)
    return dict(x=x.astype(jnp.bfloat16), k_cache=k_cache.astype(jnp.bfloat16), v_cache=v_cache.astype(jnp.bfloat16), rope_table=rope_table.astype(jnp.float32), norm_gain=norm_gain.astype(jnp.bfloat16), w_qkv=w_qkv.astype(jnp.bfloat16), b_qkv=b_qkv.astype(jnp.bfloat16), w_out=w_out.astype(jnp.bfloat16))


def apply_rotary(vals, cos_t, sin_t):
    pair_count = cos_t.shape[-1]
    lead_shape = vals.shape[:-1]
    paired = vals[..., :2 * pair_count].reshape(lead_shape + (pair_count, 2))
    even_part = paired[..., 0]
    odd_part = paired[..., 1]
    turned = jnp.stack([even_part * cos_t - odd_part * sin_t, odd_part * cos_t + even_part * sin_t], axis=-1)
    return jnp.concatenate([turned.reshape(lead_shape + (2 * pair_count,)), vals[..., 2 * pair_count:]], axis=-1)


def reference(x, k_cache, v_cache, rope_table, norm_gain, w_qkv, b_qkv, w_out):
    x_f32 = x.astype(jnp.float32)
    inv_rms = lax.rsqrt(jnp.mean(x_f32 * x_f32, axis=-1, keepdims=True) + EPS)
    hidden = (x_f32 * inv_rms * norm_gain.astype(jnp.float32)).astype(jnp.bfloat16)
    qkv_all = jnp.dot(hidden, w_qkv, preferred_element_type=jnp.float32) + b_qkv.astype(jnp.float32)
    qkv_all = qkv_all.reshape(NEW_TOKENS, KV_HEADS, GROUP + 2, HEAD)
    cos_t = rope_table[:, :PAIR_COUNT]
    sin_t = rope_table[:, PAIR_COUNT:]
    queries = apply_rotary(qkv_all[:, :, :GROUP], cos_t[:, None, None], sin_t[:, None, None]).astype(jnp.bfloat16)
    new_k = apply_rotary(qkv_all[:, :, GROUP], cos_t[:, None], sin_t[:, None]).astype(jnp.bfloat16)
    new_v = qkv_all[:, :, GROUP + 1].astype(jnp.bfloat16)
    key_count = PREFIX + NEW_TOKENS
    key_blocks = key_count // KEY_BLOCK
    keys_all = jnp.concatenate([k_cache, new_k], axis=0).reshape(key_blocks, KEY_BLOCK, KV_HEADS, HEAD)
    vals_all = jnp.concatenate([v_cache, new_v], axis=0).reshape(key_blocks, KEY_BLOCK, KV_HEADS, HEAD)
    key_pos = jnp.arange(key_count).reshape(key_blocks, KEY_BLOCK)
    q_blocks = queries.reshape(NEW_TOKENS // QUERY_BLOCK, QUERY_BLOCK, KV_HEADS, GROUP, HEAD)
    q_pos = (PREFIX + jnp.arange(NEW_TOKENS)).reshape(NEW_TOKENS // QUERY_BLOCK, QUERY_BLOCK)
    scale = HEAD ** -0.5

    def query_block(block):
        q_vals, q_at = block
        q_f32 = q_vals.astype(jnp.float32)

        def key_step(carry, kv_block):
            run_max, run_sum, weighted = carry
            k_vals, v_vals, k_at = kv_block
            scores = jnp.einsum('qngd,knd->qngk', q_f32, k_vals.astype(jnp.float32)) * scale
            visible = (k_at[None, :] <= q_at[:, None])[:, None, None, :]
            scores = jnp.where(visible, scores, MASK_VALUE)
            new_max = jnp.maximum(run_max, scores.max(axis=-1))
            rescale = jnp.exp(run_max - new_max)
            probs = jnp.exp(scores - new_max[..., None])
            run_sum = run_sum * rescale + probs.sum(axis=-1)
            weighted = weighted * rescale[..., None] + jnp.einsum('qngk,knd->qngd', probs.astype(jnp.bfloat16).astype(jnp.float32), v_vals.astype(jnp.float32))
            return (new_max, run_sum, weighted), None

        start_carry = (jnp.full((QUERY_BLOCK, KV_HEADS, GROUP), MASK_VALUE, jnp.float32), jnp.zeros((QUERY_BLOCK, KV_HEADS, GROUP), jnp.float32), jnp.zeros((QUERY_BLOCK, KV_HEADS, GROUP, HEAD), jnp.float32))
        (run_max, run_sum, weighted), _ = lax.scan(key_step, start_carry, (keys_all, vals_all, key_pos))
        return weighted / run_sum[..., None]

    attn = lax.map(query_block, (q_blocks, q_pos))
    attn = attn.reshape(NEW_TOKENS, HEADS * HEAD).astype(jnp.bfloat16)
    y = (x_f32 + jnp.dot(attn, w_out, preferred_element_type=jnp.float32)).astype(jnp.bfloat16)
    return y, new_k, new_v
```

```python
import functools
import jax
import jax.numpy as jnp
from jax import lax
from jax.experimental import pallas as pl
from jax.experimental.pallas import tpu as pltpu
from jax.sharding import PartitionSpec as P

EPS = 1.5625e-07
MASK_VALUE = -1e30
LOG2E = 1.4426950408889634
f32 = jnp.float32
bf16 = jnp.bfloat16
HEADS = 16
ROWS = 256
HEAD = 128
HALF = 128
SCALE2 = HEAD ** -0.5 * LOG2E
U = 4
ORDERS = (("x", "y", "z"), ("y", "z", "x"), ("x", "z", "y"), ("x", "y", "z"))
SUBS = 4
WIDE = 512


def proj_kernel(x_ref, g_ref, cf_ref, sf_ref, w_ref, b_ref, q_ref, k_ref, v_ref, own_ref, h_ref):
    step = pl.program_id(0)

    @pl.when(step == 0)
    def _():
        xf = x_ref[...].astype(f32)
        inv = lax.rsqrt(jnp.mean(xf * xf, axis=-1, keepdims=True) + EPS)
        h_ref[...] = (xf * inv * g_ref[...].astype(f32)).astype(bf16)

    a = jnp.dot(h_ref[...], w_ref[...], preferred_element_type=f32) + b_ref[...].astype(f32)
    lane = lax.broadcasted_iota(jnp.int32, (ROWS, HEAD), 1)

    def rope(v):
        other = jnp.where(lane % 2 == 0, pltpu.roll(v, HEAD - 1, 1), pltpu.roll(v, 1, 1))
        return v * cf_ref[...] + other * sf_ref[...]

    @pl.when(step < 8)
    def _():
        for i in range(2):
            q_ref[0, :, i * ROWS:(i + 1) * ROWS] = rope(a[:, i * HEAD:(i + 1) * HEAD]).T.astype(bf16)

    @pl.when(step == 8)
    def _():
        k = rope(a[:, :HEAD]).astype(bf16)
        v = a[:, HEAD:]
        k_ref[...] = k
        v_ref[...] = v.astype(bf16)
        vt = v.T.astype(bf16)
        for i in range(2):
            own_ref[i, 0] = k[i * HALF:(i + 1) * HALF]
            own_ref[i, 1] = vt[:, i * HALF:(i + 1) * HALF]


def project(x, norm_gain, cf, sf, w_qkv, b_qkv):
    const = lambda *shape: pl.BlockSpec(shape, lambda s: (0,) * len(shape))
    return pl.pallas_call(
        proj_kernel,
        grid=(9,),
        in_specs=[const(ROWS, 4096), const(1, 4096), const(ROWS, HEAD), const(ROWS, HEAD),
                  pl.BlockSpec((4096, 256), lambda s: (0, s)), pl.BlockSpec((1, 256), lambda s: (0, s))],
        out_specs=[pl.BlockSpec((1, HEAD, WIDE), lambda s: (jnp.minimum(s, 7), 0, 0)), const(ROWS, HEAD), const(ROWS, HEAD),
                   const(2, 2, HALF, HEAD)],
        out_shape=[jax.ShapeDtypeStruct((8, HEAD, WIDE), bf16), jax.ShapeDtypeStruct((ROWS, HEAD), bf16),
                   jax.ShapeDtypeStruct((ROWS, HEAD), bf16), jax.ShapeDtypeStruct((2, 2, HALF, HEAD), bf16)],
        scratch_shapes=[pltpu.VMEM((ROWS, 4096), bf16)],
        compiler_params=pltpu.CompilerParams(vmem_limit_bytes=48 * 2 ** 20),
        name="project",
    )(x, norm_gain.reshape(1, -1), cf, sf, w_qkv, b_qkv.reshape(1, -1))


def attn_kernel(q_ref, ownc_ref, ownn_ref, out_ref, buf, qw, acc, m, l, s, p, osend, orecv,
                snd, rcv, loc, qsem, osem):
    r = lax.axis_index("cp")
    div, rem = lax.div, lax.rem
    me = {"z": div(r, 16), "y": rem(div(r, 4), 4), "x": rem(r, 4)}
    partner = 63 - r

    def rank_of(axis, d):
        c = dict(me)
        c[axis] = rem(me[axis] + d, 4)
        return c["z"] * 16 + c["y"] * 4 + c["x"]

    def remote(src, dst, ss, rs, rank):
        return pltpu.make_async_remote_copy(src_ref=src, dst_ref=dst, send_sem=ss, recv_sem=rs, device_id={"cp": rank},
                                            device_id_type=pl.DeviceIdType.MESH)

    peers = [rank_of(a, d) for a in "xyz" for d in (1, 3)] + [rank_of("x", 2), rank_of("y", 2), partner]
    barrier = pltpu.get_barrier_semaphore()
    for peer in peers:
        pl.semaphore_signal(barrier, inc=1, device_id={"cp": peer}, device_id_type=pl.DeviceIdType.MESH)

    def place(u, c1, c2, c3):
        return 64 * u + c3 * 16 + c2 * 4 + c1

    def own_place(u):
        return buf.at[place(u, *(me[a] for a in ORDERS[u]))]

    def own_src(u):
        return ownc_ref.at[u] if u < 2 else ownn_ref.at[u - 2]

    local = [pltpu.make_async_copy(own_src(u), own_place(u), loc.at[u]) for u in range(4)]
    for c in local:
        c.start()
    qw[pl.ds(0, 4)] = q_ref[pl.ds(0, 4)]
    acc[...] = jnp.zeros_like(acc)
    l[...] = jnp.zeros_like(l)
    m[...] = jnp.full_like(m, MASK_VALUE)
    for c in local:
        c.wait()
    pl.semaphore_wait(barrier, len(peers))

    def copies(u, phase, step):
        a1, a2, a3 = ORDERS[u]
        c1, c2, c3 = (me[a] for a in ORDERS[u])
        if phase == 1:
            return [(own_src(u), own_place(u), buf.at[place(u, rem(c1 + 4 - d, 4), c2, c3)], rank_of(a1, d), n)
                    for n, d in enumerate((1, 3, 2))]
        size, axis, tag = (4, a2, 3) if phase == 2 else (16, a3, 7)

        def group(off, part=None):
            first = place(u, 0, rem(c2 + off, 4), c3) if phase == 2 else place(u, 0, 0, rem(c3 + off, 4))
            if part is None:
                return buf.at[pl.ds(first, size)]
            return buf.at[pl.ds(first + part * (size // 2), size // 2)]

        if step == 1:
            return [(group(0), group(0), group(3), rank_of(axis, 1), tag),
                    (group(0), group(0), group(1), rank_of(axis, 3), tag + 1)]
        return [(group(3, 0), group(3, 0), group(2, 0), rank_of(axis, 1), tag + 2),
                (group(1, 1), group(1, 1), group(2, 1), rank_of(axis, 3), tag + 3)]

    def start(units, phase, step=1):
        for u in units:
            for src, dst, _, rank, tag in copies(u, phase, step):
                remote(src, dst, snd.at[u, tag], rcv.at[u, tag], rank).start()

    def arrived(units, phase, step=1):
        for u in units:
            for src, dst, got, rank, tag in copies(u, phase, step):
                remote(got, got, snd.at[u, tag], rcv.at[u, tag], rank).wait_recv()

    def sent(units, phase, step=1):
        for u in units:
            for src, dst, got, rank, tag in copies(u, phase, step):
                remote(src, dst, snd.at[u, tag], rcv.at[u, tag], rank).wait_send()

    cache, new = (0, 1), (2, 3)
    start(cache, 1)
    q_copy = remote(q_ref.at[pl.ds(4, 4)], qw.at[pl.ds(4, 4)], qsem.at[0], qsem.at[1], partner)
    q_copy.start()
    arrived(cache, 1)
    start(cache, 2, 1)
    arrived(cache, 2, 1)
    start(cache, 2, 2)
    start(new, 1)
    arrived(cache, 2, 2)
    start(cache, 3, 1)
    q_copy.wait()

    def event(b):
        @pl.when(b == 2)
        def _():
            arrived(new, 1)
            start(new, 2, 1)

        @pl.when(b == 7)
        def _():
            arrived(cache, 3, 1)
            start(cache, 3, 2)
            arrived(new, 2, 1)
            start(new, 2, 2)

        @pl.when(b == 12)
        def _():
            arrived(new, 2, 2)
            start(new, 3, 1)

        @pl.when(b == 22)
        def _():
            arrived(new, 3, 1)
            start(new, 3, 2)

        @pl.when(b == 23)
        def _():
            arrived(cache, 3, 2)

        @pl.when(b == 27)
        def _():
            arrived(new, 3, 2)

    def cache_desc(chunk, prb):
        g, cg = div(chunk, 4), rem(chunk, 4)
        off = g + jnp.where(g == 2, 1, 0) - jnp.where(g == 3, 1, 0)
        plane = rem(jnp.where(cg < 2, me["z"], me["x"]) + off, 4)
        base = plane * 16 + jnp.where(cg < 2, 0, 64) + rem(cg, 2) * 8
        return base, base + 1, jnp.int32(2), prb

    def new_desc(c, prb):
        return 128 + rem(c, 4) * 16 + div(c, 4) * 4, 192 + 4 * c, jnp.int32(1), prb

    def pick(cond, a, b):
        return tuple(lax.select(cond, i, j) for i, j in zip(a, b))

    def desc_first(b):
        c1 = cache_desc(div(b, 2), 4 * rem(b, 2))
        c2 = cache_desc(12 + (b - 24), jnp.int32(4))
        c3 = new_desc(b - 28, jnp.int32(4))
        return pick(b < 24, c1, pick(b < 28, c2, c3))

    def desc_second(b):
        return pick(b < 4, cache_desc(12 + b, jnp.int32(0)), new_desc(b - 4, jnp.int32(0)))

    def scores(d, u, i, mx, mask):
        kk = jnp.concatenate([buf[d[0] + i * d[2], 0], buf[d[1] + i * d[2], 0]], axis=0)
        st = jnp.dot(kk, qw[d[3] + u], preferred_element_type=f32)
        if mask is not None:
            st = jnp.where(mask(i), st, MASK_VALUE)
        s[i * 256:(i + 1) * 256, :] = st
        t = jnp.max(st.reshape(32, 8, WIDE), axis=0)
        return t if mx is None else jnp.maximum(mx, t)

    def run(desc, bodies, mask=None, on_body=None):
        def at(b):
            return desc(jnp.minimum(b, bodies - 1))

        def step(d, dn, u, mx8):
            pr = d[3] + u
            nxt, un = (d, u + 1) if u + 1 < U else (dn, 0)
            mx = jnp.max(mx8, axis=0, keepdims=True) * SCALE2
            mo = m[pr]
            mn = jnp.maximum(mo, mx)
            alpha = jnp.exp2(mo - mn)
            m[pr] = mn
            ls = l[pr] * alpha
            weighted, mxn = None, None
            for i in range(SUBS):
                e = jnp.exp2(s[i * 256:(i + 1) * 256, :] * SCALE2 - mn)
                ls = ls + jnp.sum(e.reshape(32, 8, WIDE), axis=0)
                p[i % 2] = e.astype(bf16)
                mxn = scores(nxt, un, i, mxn, mask)
                vv = jnp.concatenate([buf[d[0] + i * d[2], 1], buf[d[1] + i * d[2], 1]], axis=1)
                part = jnp.dot(vv, p[i % 2], preferred_element_type=f32)
                weighted = part if weighted is None else weighted + part
            l[pr] = ls
            acc[pr] = acc[pr] * alpha + weighted
            return mxn

        d0 = at(jnp.int32(0))
        mx = None
        for i in range(SUBS):
            mx = scores(d0, 0, i, mx, mask)

        def body(b, mx):
            if on_body is not None:
                on_body(b)
            d, dn = at(b), at(b + 1)
            for u in range(U):
                mx = step(d, dn, u, mx)
            return mx

        lax.fori_loop(0, bodies, body, mx)

    def diagonal(rank, prb):
        c = div(rank, SUBS)

        def mask(i):
            key = (SUBS * c + i) * ROWS + lax.broadcasted_iota(jnp.int32, (256, WIDE), 0)
            return key <= rank * ROWS + (lax.broadcasted_iota(jnp.int32, (256, WIDE), 1) & (ROWS - 1))

        run(lambda b: new_desc(c, jnp.int32(prb)), 1, mask)

    def result(pr):
        return (acc[pr] / jnp.sum(l[pr], axis=0, keepdims=True)).astype(bf16)

    run(desc_first, 28 + div(partner, SUBS), on_body=event)
    diagonal(partner, 4)
    for h in range(4):
        osend[h] = result(4 + h)
    o_copy = remote(osend, orecv, osem.at[0], osem.at[1], partner)
    o_copy.start()
    run(desc_second, 4 + div(r, SUBS))
    diagonal(r, 0)
    for h in range(4):
        res = result(h)
        for q in range(2):
            out_ref[2 * h + q] = res[:, q * ROWS:(q + 1) * ROWS]
    o_copy.wait()
    for h in range(4):
        for q in range(2):
            out_ref[8 + 2 * h + q] = orecv[h, :, q * ROWS:(q + 1) * ROWS]

    for units in (cache, new):
        sent(units, 1)
        for phase in (2, 3):
            for step in (1, 2):
                sent(units, phase, step)


def attend(q, own_cache, own_new):
    vm = pl.BlockSpec(memory_space=pltpu.VMEM)
    return pl.pallas_call(
        attn_kernel,
        out_shape=jax.ShapeDtypeStruct((HEADS, HEAD, ROWS), bf16),
        in_specs=[vm] * 3,
        out_specs=vm,
        scratch_shapes=[
            pltpu.VMEM((256, 2, HALF, HEAD), bf16),
            pltpu.VMEM((8, HEAD, WIDE), bf16),
            pltpu.VMEM((8, HEAD, WIDE), f32),
            pltpu.VMEM((8, 1, WIDE), f32),
            pltpu.VMEM((8, 8, WIDE), f32),
            pltpu.VMEM((SUBS * 256, WIDE), f32),
            pltpu.VMEM((2, 256, WIDE), bf16),
            pltpu.VMEM((4, HEAD, WIDE), bf16),
            pltpu.VMEM((4, HEAD, WIDE), bf16),
            pltpu.SemaphoreType.DMA((4, 11)),
            pltpu.SemaphoreType.DMA((4, 11)),
            pltpu.SemaphoreType.DMA((4,)),
            pltpu.SemaphoreType.DMA((2,)),
            pltpu.SemaphoreType.DMA((2,)),
        ],
        compiler_params=pltpu.CompilerParams(collective_id=0, has_side_effects=True, vmem_limit_bytes=48 * 2 ** 20),
        name="attend",
    )(q, own_cache, own_new)


def local_step(x, k_cache, v_cache, rope_table, norm_gain, w_qkv, b_qkv, w_out):
    cos_t, sin_t = rope_table[:, :32], rope_table[:, 32:]
    cf = jnp.concatenate([jnp.repeat(cos_t, 2, axis=1), jnp.ones((ROWS, 64), f32)], axis=1)
    sf = jnp.concatenate([jnp.stack([-sin_t, sin_t], axis=-1).reshape(ROWS, 64), jnp.zeros((ROWS, 64), f32)], axis=1)
    q, new_k, new_v, own_new = project(x, norm_gain, cf, sf, w_qkv, b_qkv)
    kc = k_cache.reshape(2, HALF, HEAD)
    vc = v_cache.reshape(2, HALF, HEAD).transpose(0, 2, 1)
    own_cache = jnp.stack([kc, vc], axis=1)
    o_t = attend(q, own_cache, own_new)
    o = o_t.reshape(HEADS * HEAD, ROWS)
    x_f32 = x.astype(f32)
    parts = []
    for c in range(4):
        cols = slice(c * 1024, (c + 1) * 1024)
        part = lax.dot_general(o, w_out[:, cols], (((0,), (0,)), ((), ())), preferred_element_type=f32)
        other = lax.ppermute(part, "tp", [(0, 1), (1, 0)])
        parts.append((x_f32[:, cols] + (part + other)).astype(bf16))
    y = jnp.concatenate(parts, axis=1)
    return y, new_k.reshape(ROWS, 1, HEAD), new_v.reshape(ROWS, 1, HEAD)


def solution(mesh):
    row_spec = P(('dp', 'cp'), None)
    cache_spec = P(('dp', 'cp'), 'tp', None)
    step = jax.shard_map(local_step, mesh=mesh, in_specs=(row_spec, cache_spec, cache_spec, row_spec, P(None), P(None, 'tp'), P('tp'), P('tp', None)), out_specs=(row_spec, cache_spec, cache_spec), check_vma=False)

    def run(*args):
        with jax.sharding.use_abstract_mesh(mesh.abstract_mesh):
            return step(*args)
    return run
```

```python
import functools
import jax
import jax.numpy as jnp
from jax import lax
from jax.experimental import pallas as pl
from jax.experimental.pallas import tpu as pltpu
from jax.sharding import PartitionSpec as P

EPS = 1.5625e-07
MASK_VALUE = -1e30
LOG2E = 1.4426950408889634
f32 = jnp.float32
bf16 = jnp.bfloat16
HEADS = 16
ROWS = 256
HEAD = 128
HALF = 128
SCALE2 = HEAD ** -0.5 * LOG2E
U = 4
ORDERS = (("x", "y", "z"), ("y", "z", "x"), ("x", "z", "y"), ("x", "y", "z"))
SUBS = 4
WIDE = 512


def proj_kernel(x_ref, g_ref, cf_ref, sf_ref, w_ref, b_ref, q_ref, k_ref, v_ref, own_ref, h_ref):
    step = pl.program_id(0)

    @pl.when(step == 0)
    def _():
        xf = x_ref[...].astype(f32)
        inv = lax.rsqrt(jnp.mean(xf * xf, axis=-1, keepdims=True) + EPS)
        h_ref[...] = (xf * inv * g_ref[...].astype(f32)).astype(bf16)

    a = jnp.dot(h_ref[...], w_ref[...], preferred_element_type=f32) + b_ref[...].astype(f32)
    lane = lax.broadcasted_iota(jnp.int32, (ROWS, HEAD), 1)

    def rope(v):
        other = jnp.where(lane % 2 == 0, pltpu.roll(v, HEAD - 1, 1), pltpu.roll(v, 1, 1))
        return v * cf_ref[...] + other * sf_ref[...]

    @pl.when(step < 8)
    def _():
        for i in range(2):
            q_ref[0, :, i * ROWS:(i + 1) * ROWS] = rope(a[:, i * HEAD:(i + 1) * HEAD]).T.astype(bf16)

    @pl.when(step == 8)
    def _():
        k = rope(a[:, :HEAD]).astype(bf16)
        v = a[:, HEAD:]
        k_ref[...] = k
        v_ref[...] = v.astype(bf16)
        vt = v.T.astype(bf16)
        for i in range(2):
            own_ref[i, 0] = k[i * HALF:(i + 1) * HALF]
            own_ref[i, 1] = vt[:, i * HALF:(i + 1) * HALF]


def project(x, norm_gain, cf, sf, w_qkv, b_qkv):
    const = lambda *shape: pl.BlockSpec(shape, lambda s: (0,) * len(shape))
    return pl.pallas_call(
        proj_kernel,
        grid=(9,),
        in_specs=[const(ROWS, 4096), const(1, 4096), const(ROWS, HEAD), const(ROWS, HEAD),
                  pl.BlockSpec((4096, 256), lambda s: (0, s)), pl.BlockSpec((1, 256), lambda s: (0, s))],
        out_specs=[pl.BlockSpec((1, HEAD, WIDE), lambda s: (jnp.minimum(s, 7), 0, 0)), const(ROWS, HEAD), const(ROWS, HEAD),
                   const(2, 2, HALF, HEAD)],
        out_shape=[jax.ShapeDtypeStruct((8, HEAD, WIDE), bf16), jax.ShapeDtypeStruct((ROWS, HEAD), bf16),
                   jax.ShapeDtypeStruct((ROWS, HEAD), bf16), jax.ShapeDtypeStruct((2, 2, HALF, HEAD), bf16)],
        scratch_shapes=[pltpu.VMEM((ROWS, 4096), bf16)],
        compiler_params=pltpu.CompilerParams(vmem_limit_bytes=48 * 2 ** 20),
        name="project",
    )(x, norm_gain.reshape(1, -1), cf, sf, w_qkv, b_qkv.reshape(1, -1))


def attn_kernel(q_ref, ownc_ref, ownn_ref, out_ref, buf, qw, acc, m, l, s, p, osend, orecv,
                snd, rcv, loc, qsem, osem):
    r = lax.axis_index("cp")
    div, rem = lax.div, lax.rem
    me = {"z": div(r, 16), "y": rem(div(r, 4), 4), "x": rem(r, 4)}
    partner = 63 - r

    def rank_of(axis, d):
        c = dict(me)
        c[axis] = rem(me[axis] + d, 4)
        return c["z"] * 16 + c["y"] * 4 + c["x"]

    def remote(src, dst, ss, rs, rank):
        return pltpu.make_async_remote_copy(src_ref=src, dst_ref=dst, send_sem=ss, recv_sem=rs, device_id={"cp": rank},
                                            device_id_type=pl.DeviceIdType.MESH)

    peers = [rank_of(a, d) for a in "xyz" for d in (1, 3)] + [rank_of("x", 2), rank_of("y", 2), partner]
    barrier = pltpu.get_barrier_semaphore()
    for peer in peers:
        pl.semaphore_signal(barrier, inc=1, device_id={"cp": peer}, device_id_type=pl.DeviceIdType.MESH)

    def place(u, c1, c2, c3):
        return 64 * u + c3 * 16 + c2 * 4 + c1

    def own_place(u):
        return buf.at[place(u, *(me[a] for a in ORDERS[u]))]

    def own_src(u):
        return ownc_ref.at[u] if u < 2 else ownn_ref.at[u - 2]

    local = [pltpu.make_async_copy(own_src(u), own_place(u), loc.at[u]) for u in range(4)]
    for c in local:
        c.start()
    qw[pl.ds(0, 4)] = q_ref[pl.ds(0, 4)]
    acc[...] = jnp.zeros_like(acc)
    l[...] = jnp.zeros_like(l)
    m[...] = jnp.full_like(m, MASK_VALUE)
    for c in local:
        c.wait()
    pl.semaphore_wait(barrier, len(peers))

    def copies(u, phase, step):
        a1, a2, a3 = ORDERS[u]
        c1, c2, c3 = (me[a] for a in ORDERS[u])
        if phase == 1:
            return [(own_src(u), own_place(u), buf.at[place(u, rem(c1 + 4 - d, 4), c2, c3)], rank_of(a1, d), n)
                    for n, d in enumerate((1, 3, 2))]
        size, axis, tag = (4, a2, 3) if phase == 2 else (16, a3, 7)

        def group(off, part=None):
            first = place(u, 0, rem(c2 + off, 4), c3) if phase == 2 else place(u, 0, 0, rem(c3 + off, 4))
            if part is None:
                return buf.at[pl.ds(first, size)]
            return buf.at[pl.ds(first + part * (size // 2), size // 2)]

        up, down = rank_of(axis, 1), rank_of(axis, 3)
        if step == 1 and phase == 2:
            return [(group(0), group(0), group(3), up, tag), (group(0), group(0), group(1), down, tag + 1)]
        if step < 2:
            h = int(2 * step)
            return [(group(0, h), group(0, h), group(3, h), up, tag + 2 * h),
                    (group(0, h), group(0, h), group(1, h), down, tag + 2 * h + 1)]
        out = [(group(3, 0), group(3, 0), group(2, 0), up, tag + 2 + size // 8),
               (group(1, 1), group(1, 1), group(2, 1), down, tag + 3 + size // 8)]
        return out if step == 2 else [out[int(step) - 3]]

    def start(units, phase, step=1):
        for u in units:
            for src, dst, _, rank, tag in copies(u, phase, step):
                remote(src, dst, snd.at[u, tag], rcv.at[u, tag], rank).start()

    def arrived(units, phase, step=1):
        for u in units:
            for src, dst, got, rank, tag in copies(u, phase, step):
                remote(got, got, snd.at[u, tag], rcv.at[u, tag], rank).wait_recv()

    def sent(units, phase, step=1):
        for u in units:
            for src, dst, got, rank, tag in copies(u, phase, step):
                remote(src, dst, snd.at[u, tag], rcv.at[u, tag], rank).wait_send()

    cache, new = (0, 1), (2, 3)
    q_copy = remote(q_ref.at[pl.ds(4, 4)], qw.at[pl.ds(4, 4)], qsem.at[0], qsem.at[1], partner)
    start(cache, 1)
    q_copy.start()
    arrived(cache, 1)
    start(cache, 2, 1)
    start(new, 1)
    arrived(cache, 2, 1)
    start(cache, 2, 2)
    arrived(new, 1)
    start(new, 2, 1)
    arrived(cache, 2, 2)
    start(cache, 3, 0)
    start(cache, 3, 0.5)

    def event(at):
        @pl.when(at == 3)
        def _():
            q_copy.wait()
            arrived(new, 2, 1)
            start(new, 2, 2)

        @pl.when(at == 7)
        def _():
            arrived(cache, 3, 0)
            start(cache, 3, 3)

        @pl.when(at == 8)
        def _():
            arrived(new, 2, 2)
            start(new, 3, 0)
            start(new, 3, 0.5)

        @pl.when(at == 15)
        def _():
            arrived(cache, 3, 0.5)
            start(cache, 3, 4)

        @pl.when(at == 23)
        def _():
            arrived(cache, 3, 2)
            arrived(new, 3, 0)
            arrived(new, 3, 0.5)
            start(new, 3, 2)

        @pl.when(at == 27)
        def _():
            arrived(new, 3, 2)

    def cache_desc(chunk, prb):
        g, cg = div(chunk, 4), rem(chunk, 4)
        second = rem(cg, 2)
        near = (g == 1) | (g == 2)
        off = jnp.where(near, 1 + 2 * second, jnp.where(g == 0, 0, 2))
        half = jnp.where(near, g - 1, second)
        plane = rem(jnp.where(cg < 2, me["z"], me["x"]) + off, 4)
        base = plane * 16 + jnp.where(cg < 2, 0, 64) + half * 8
        return base, base + 4, prb

    def new_desc(c, prb):
        return 128 + rem(c, 4) * 16 + div(c, 4) * 4, 192 + 4 * c, prb

    def pick(cond, a, b):
        return tuple(lax.select(cond, i, j) for i, j in zip(a, b))

    def desc_first(b):
        c1 = cache_desc(4 * div(b, 8) + rem(b, 4), 4 * rem(div(b, 4), 2))
        c2 = cache_desc(12 + (b - 24), jnp.int32(4))
        c3 = new_desc(b - 28, jnp.int32(4))
        return pick(b < 24, c1, pick(b < 28, c2, c3))

    def desc_second(b):
        return pick(b < 4, cache_desc(12 + b, jnp.int32(0)), new_desc(b - 4, jnp.int32(0)))

    def desc_of(turn, b):
        return pick(turn == 0, desc_first(b), desc_second(b))

    def scores(d, u, i, mx):
        run4, j = buf.at[pl.ds(d[i // 2], 4)], 2 * (i % 2)
        kk = jnp.concatenate([run4[j, 0], run4[j + 1, 0]], axis=0)
        st = jnp.dot(kk, qw[d[2] + u], preferred_element_type=f32)
        s[i * 256:(i + 1) * 256, :] = st
        t = jnp.max(st.reshape(32, 8, WIDE), axis=0)
        return t if mx is None else jnp.maximum(mx, t)

    def step(d, dn, u, mx8):
        pr = d[2] + u
        nxt, un = (d, u + 1) if u + 1 < U else (dn, 0)
        mx = jnp.max(mx8, axis=0, keepdims=True) * SCALE2
        mo = m[pr]
        mn = jnp.maximum(mo, mx)
        alpha = jnp.exp2(mo - mn)
        m[pr] = mn
        ls = l[pr] * alpha
        weighted, mxn = None, None
        for i in range(SUBS):
            e = jnp.exp2(s[i * 256:(i + 1) * 256, :] * SCALE2 - mn)
            ls = ls + jnp.sum(e.reshape(32, 8, WIDE), axis=0)
            p[i % 2] = e.astype(bf16)
            mxn = scores(nxt, un, i, mxn)
            run4, j = buf.at[pl.ds(d[i // 2], 4)], 2 * (i % 2)
            vv = jnp.concatenate([run4[j, 1], run4[j + 1, 1]], axis=1)
            part = jnp.dot(vv, p[i % 2], preferred_element_type=f32)
            weighted = part if weighted is None else weighted + part
        l[pr] = ls
        acc[pr] = acc[pr] * alpha + weighted
        return mxn

    def masked_block(rank, prb, block):
        f = 128 + rem(div(block, 4), 4) * 16 + div(block, 16) * 4 + rem(block, 4)
        g = 192 + block
        key = block * ROWS + lax.broadcasted_iota(jnp.int32, (256, WIDE), 0)
        seen = key <= rank * ROWS + (lax.broadcasted_iota(jnp.int32, (256, WIDE), 1) & (ROWS - 1))
        kk = jnp.concatenate([buf[f, 0], buf[g, 0]], axis=0)
        vv = jnp.concatenate([buf[f, 1], buf[g, 1]], axis=1)
        for u in range(4):
            pr = prb + u
            st = jnp.where(seen, jnp.dot(kk, qw[pr], preferred_element_type=f32), MASK_VALUE)
            mx = jnp.max(jnp.max(st.reshape(32, 8, WIDE), axis=0), axis=0, keepdims=True) * SCALE2
            mo = m[pr]
            mn = jnp.maximum(mo, mx)
            alpha = jnp.exp2(mo - mn)
            m[pr] = mn
            e = jnp.exp2(st * SCALE2 - mn)
            l[pr] = l[pr] * alpha + jnp.sum(e.reshape(32, 8, WIDE), axis=0)
            acc[pr] = acc[pr] * alpha + jnp.dot(vv, e.astype(bf16), preferred_element_type=f32)

    o_copy = remote(osend, orecv, osem.at[0], osem.at[1], partner)

    def turn_body(turn, carry):
        rank = lax.select(turn == 0, partner, r)
        bodies = lax.select(turn == 0, jnp.int32(28), jnp.int32(4)) + div(rank, SUBS)
        prb = lax.select(turn == 0, jnp.int32(4), jnp.int32(0))
        d0 = desc_of(turn, jnp.int32(0))
        mx = None
        for i in range(SUBS):
            mx = scores(d0, 0, i, mx)

        def body(b, mx):
            event(b + 1000 * turn)
            d, dn = desc_of(turn, b), desc_of(turn, jnp.minimum(b + 1, bodies - 1))
            for u in range(U):
                mx = step(d, dn, u, mx)
            return mx

        lax.fori_loop(0, bodies, body, mx)
        start_block = rank - rem(rank, SUBS)

        def tail(j, carry):
            masked_block(rank, prb, start_block + j)
            return carry

        lax.fori_loop(0, rem(rank, SUBS) + 1, tail, 0)

        def result(h, carry):
            res = (acc[prb + h] / jnp.sum(l[prb + h], axis=0, keepdims=True)).T.astype(bf16)

            @pl.when(turn == 0)
            def _():
                osend[h] = res

            @pl.when(turn == 1)
            def _():
                out_ref[h] = res

            return carry

        lax.fori_loop(0, 4, result, 0)

        @pl.when(turn == 0)
        def _():
            o_copy.start()

        return carry

    lax.fori_loop(0, 2, turn_body, 0)
    o_copy.wait()
    out_ref[pl.ds(4, 4)] = orecv[...]

    for units in (cache, new):
        for phase, step in ((1, 1), (2, 1), (2, 2), (3, 0), (3, 0.5), (3, 2)):
            sent(units, phase, step)


def attend(q, own_cache, own_new):
    vm = pl.BlockSpec(memory_space=pltpu.VMEM)
    return pl.pallas_call(
        attn_kernel,
        out_shape=jax.ShapeDtypeStruct((8, WIDE, HEAD), bf16),
        in_specs=[vm] * 3,
        out_specs=vm,
        scratch_shapes=[
            pltpu.VMEM((256, 2, HALF, HEAD), bf16),
            pltpu.VMEM((8, HEAD, WIDE), bf16),
            pltpu.VMEM((8, HEAD, WIDE), f32),
            pltpu.VMEM((8, 1, WIDE), f32),
            pltpu.VMEM((8, 8, WIDE), f32),
            pltpu.VMEM((SUBS * 256, WIDE), f32),
            pltpu.VMEM((2, 256, WIDE), bf16),
            pltpu.VMEM((4, WIDE, HEAD), bf16),
            pltpu.VMEM((4, WIDE, HEAD), bf16),
            pltpu.SemaphoreType.DMA((4, 13)),
            pltpu.SemaphoreType.DMA((4, 13)),
            pltpu.SemaphoreType.DMA((4,)),
            pltpu.SemaphoreType.DMA((2,)),
            pltpu.SemaphoreType.DMA((2,)),
        ],
        compiler_params=pltpu.CompilerParams(collective_id=0, has_side_effects=True, vmem_limit_bytes=48 * 2 ** 20),
        name="attend",
    )(q, own_cache, own_new)


TILE = 512
TILES = 4096 // TILE


def out_kernel(o_ref, w_ref, x_ref, y_ref, o_s, mine, other, snd, rcv):
    step = pl.program_id(0)
    peer = 1 - lax.axis_index("tp")

    def copy(j):
        return pltpu.make_async_remote_copy(src_ref=mine.at[j], dst_ref=other.at[j], send_sem=snd.at[j], recv_sem=rcv.at[j],
                                            device_id={"tp": peer}, device_id_type=pl.DeviceIdType.MESH)

    @pl.when(step == 0)
    def _():
        barrier = pltpu.get_barrier_semaphore()
        pl.semaphore_signal(barrier, inc=1, device_id={"tp": peer}, device_id_type=pl.DeviceIdType.MESH)
        for h in range(HEADS):
            o_s[:, h * HEAD:(h + 1) * HEAD] = o_ref[h // 2, (h % 2) * ROWS:(h % 2 + 1) * ROWS, :]
        pl.semaphore_wait(barrier, 1)

    @pl.when(step < TILES)
    def _():
        mine[step] = jnp.dot(o_s[...], w_ref[...], preferred_element_type=f32)
        copy(step).start()

    @pl.when(step > 0)
    def _():
        copy(step - 1).wait()
        y_ref[...] = (x_ref[...].astype(f32) + (mine[step - 1] + other[step - 1])).astype(bf16)


def out_project(o, w_out, x):
    late = lambda j: (0, jnp.maximum(j - 1, 0))
    return pl.pallas_call(
        out_kernel,
        grid=(TILES + 1,),
        in_specs=[pl.BlockSpec((8, WIDE, HEAD), lambda j: (0, 0, 0)),
                  pl.BlockSpec((HEADS * HEAD, TILE), lambda j: (0, jnp.minimum(j, TILES - 1))),
                  pl.BlockSpec((ROWS, TILE), late)],
        out_specs=pl.BlockSpec((ROWS, TILE), late),
        out_shape=jax.ShapeDtypeStruct((ROWS, 4096), bf16),
        scratch_shapes=[pltpu.VMEM((ROWS, HEADS * HEAD), bf16), pltpu.VMEM((TILES, ROWS, TILE), f32),
                        pltpu.VMEM((TILES, ROWS, TILE), f32), pltpu.SemaphoreType.DMA((TILES,)), pltpu.SemaphoreType.DMA((TILES,))],
        compiler_params=pltpu.CompilerParams(collective_id=1, has_side_effects=True, vmem_limit_bytes=48 * 2 ** 20),
        name="outproj",
    )(o, w_out, x)


def local_step(x, k_cache, v_cache, rope_table, norm_gain, w_qkv, b_qkv, w_out):
    cos_t, sin_t = rope_table[:, :32], rope_table[:, 32:]
    cf = jnp.concatenate([jnp.repeat(cos_t, 2, axis=1), jnp.ones((ROWS, 64), f32)], axis=1)
    sf = jnp.concatenate([jnp.stack([-sin_t, sin_t], axis=-1).reshape(ROWS, 64), jnp.zeros((ROWS, 64), f32)], axis=1)
    q, new_k, new_v, own_new = project(x, norm_gain, cf, sf, w_qkv, b_qkv)
    kc = k_cache.reshape(2, HALF, HEAD)
    vc = v_cache.reshape(2, HALF, HEAD).transpose(0, 2, 1)
    own_cache = jnp.stack([kc, vc], axis=1)
    o = attend(q, own_cache, own_new)
    y = out_project(o, w_out, x)
    return y, new_k.reshape(ROWS, 1, HEAD), new_v.reshape(ROWS, 1, HEAD)


def solution(mesh):
    row_spec = P(('dp', 'cp'), None)
    cache_spec = P(('dp', 'cp'), 'tp', None)
    step = jax.shard_map(local_step, mesh=mesh, in_specs=(row_spec, cache_spec, cache_spec, row_spec, P(None), P(None, 'tp'), P('tp'), P('tp', None)), out_specs=(row_spec, cache_spec, cache_spec), check_vma=False)

    def run(*args):
        with jax.sharding.use_abstract_mesh(mesh.abstract_mesh):
            return step(*args)
    return run
```

```python
import functools
import jax
import jax.numpy as jnp
from jax import lax
from jax.experimental import pallas as pl
from jax.experimental.pallas import tpu as pltpu
from jax.sharding import PartitionSpec as P

EPS = 1.5625e-07
MASK_VALUE = -1e30
LOG2E = 1.4426950408889634
f32 = jnp.float32
bf16 = jnp.bfloat16
HEADS = 16
ROWS = 256
HEAD = 128
HALF = 128
SCALE2 = HEAD ** -0.5 * LOG2E
U = 4
ORDERS = (("x", "y", "z"), ("y", "z", "x"), ("x", "z", "y"), ("x", "y", "z"))
SUBS = 4
WIDE = 512


def proj_kernel(x_ref, g_ref, cf_ref, sf_ref, w_ref, b_ref, q_ref, k_ref, v_ref, own_ref, h_ref):
    step = pl.program_id(0)

    @pl.when(step == 0)
    def _():
        xf = x_ref[...].astype(f32)
        inv = lax.rsqrt(jnp.mean(xf * xf, axis=-1, keepdims=True) + EPS)
        h_ref[...] = (xf * inv * g_ref[...].astype(f32)).astype(bf16)

    a = jnp.dot(h_ref[...], w_ref[...], preferred_element_type=f32) + b_ref[...].astype(f32)
    lane = lax.broadcasted_iota(jnp.int32, (ROWS, HEAD), 1)

    def rope(v):
        other = jnp.where(lane % 2 == 0, pltpu.roll(v, HEAD - 1, 1), pltpu.roll(v, 1, 1))
        return v * cf_ref[...] + other * sf_ref[...]

    @pl.when(step < 8)
    def _():
        for i in range(2):
            q_ref[0, :, i * ROWS:(i + 1) * ROWS] = rope(a[:, i * HEAD:(i + 1) * HEAD]).T.astype(bf16)

    @pl.when(step == 8)
    def _():
        k = rope(a[:, :HEAD]).astype(bf16)
        v = a[:, HEAD:]
        k_ref[...] = k
        v_ref[...] = v.astype(bf16)
        vt = v.T.astype(bf16)
        for i in range(2):
            own_ref[i, 0] = k[i * HALF:(i + 1) * HALF]
            own_ref[i, 1] = vt[:, i * HALF:(i + 1) * HALF]


def project(x, norm_gain, cf, sf, w_qkv, b_qkv):
    const = lambda *shape: pl.BlockSpec(shape, lambda s: (0,) * len(shape))
    return pl.pallas_call(
        proj_kernel,
        grid=(9,),
        in_specs=[const(ROWS, 4096), const(1, 4096), const(ROWS, HEAD), const(ROWS, HEAD),
                  pl.BlockSpec((4096, 256), lambda s: (0, s)), pl.BlockSpec((1, 256), lambda s: (0, s))],
        out_specs=[pl.BlockSpec((1, HEAD, WIDE), lambda s: (jnp.minimum(s, 7), 0, 0)), const(ROWS, HEAD), const(ROWS, HEAD),
                   const(2, 2, HALF, HEAD)],
        out_shape=[jax.ShapeDtypeStruct((8, HEAD, WIDE), bf16), jax.ShapeDtypeStruct((ROWS, HEAD), bf16),
                   jax.ShapeDtypeStruct((ROWS, HEAD), bf16), jax.ShapeDtypeStruct((2, 2, HALF, HEAD), bf16)],
        scratch_shapes=[pltpu.VMEM((ROWS, 4096), bf16)],
        compiler_params=pltpu.CompilerParams(vmem_limit_bytes=48 * 2 ** 20),
        name="project",
    )(x, norm_gain.reshape(1, -1), cf, sf, w_qkv, b_qkv.reshape(1, -1))


def attn_kernel(q_ref, ownc_ref, ownn_ref, out_ref, buf, qw, acc, m, l, s, p, osend, orecv,
                snd, rcv, loc, qsem, osem):
    r = lax.axis_index("cp")
    div, rem = lax.div, lax.rem
    me = {"z": div(r, 16), "y": rem(div(r, 4), 4), "x": rem(r, 4)}
    partner = 63 - r

    def rank_of(axis, d):
        c = dict(me)
        c[axis] = rem(me[axis] + d, 4)
        return c["z"] * 16 + c["y"] * 4 + c["x"]

    def remote(src, dst, ss, rs, rank):
        return pltpu.make_async_remote_copy(src_ref=src, dst_ref=dst, send_sem=ss, recv_sem=rs, device_id={"cp": rank},
                                            device_id_type=pl.DeviceIdType.MESH)

    peers = [rank_of(a, d) for a in "xyz" for d in (1, 3)] + [rank_of("x", 2), rank_of("y", 2), partner]
    barrier = pltpu.get_barrier_semaphore()
    for peer in peers:
        pl.semaphore_signal(barrier, inc=1, device_id={"cp": peer}, device_id_type=pl.DeviceIdType.MESH)

    def place(u, c1, c2, c3):
        return 64 * u + c3 * 16 + c2 * 4 + c1

    def own_place(u):
        return buf.at[place(u, *(me[a] for a in ORDERS[u]))]

    def own_src(u):
        return ownc_ref.at[u] if u < 2 else ownn_ref.at[u - 2]

    local = [pltpu.make_async_copy(own_src(u), own_place(u), loc.at[u]) for u in range(4)]
    for c in local:
        c.start()
    qw[pl.ds(0, 4)] = q_ref[pl.ds(0, 4)]
    acc[...] = jnp.zeros_like(acc)
    l[...] = jnp.zeros_like(l)
    m[...] = jnp.full_like(m, MASK_VALUE)
    for c in local:
        c.wait()
    pl.semaphore_wait(barrier, len(peers))

    def copies(u, phase, step):
        a1, a2, a3 = ORDERS[u]
        c1, c2, c3 = (me[a] for a in ORDERS[u])
        if phase == 1:
            return [(own_src(u), own_place(u), buf.at[place(u, rem(c1 + 4 - d, 4), c2, c3)], rank_of(a1, d), n)
                    for n, d in enumerate((1, 3, 2))]
        size, axis, tag = (4, a2, 3) if phase == 2 else (16, a3, 7)

        def group(off, part=None):
            first = place(u, 0, rem(c2 + off, 4), c3) if phase == 2 else place(u, 0, 0, rem(c3 + off, 4))
            if part is None:
                return buf.at[pl.ds(first, size)]
            return buf.at[pl.ds(first + part * (size // 2), size // 2)]

        up, down = rank_of(axis, 1), rank_of(axis, 3)
        if step == 1 and phase == 2:
            return [(group(0), group(0), group(3), up, tag), (group(0), group(0), group(1), down, tag + 1)]
        if step < 2:
            h = int(2 * step)
            return [(group(0, h), group(0, h), group(3, h), up, tag + 2 * h),
                    (group(0, h), group(0, h), group(1, h), down, tag + 2 * h + 1)]
        out = [(group(3, 0), group(3, 0), group(2, 0), up, tag + 2 + size // 8),
               (group(1, 1), group(1, 1), group(2, 1), down, tag + 3 + size // 8)]
        return out if step == 2 else [out[int(step) - 3]]

    def start(units, phase, step=1):
        for u in units:
            for src, dst, _, rank, tag in copies(u, phase, step):
                remote(src, dst, snd.at[u, tag], rcv.at[u, tag], rank).start()

    def arrived(units, phase, step=1):
        for u in units:
            for src, dst, got, rank, tag in copies(u, phase, step):
                remote(got, got, snd.at[u, tag], rcv.at[u, tag], rank).wait_recv()

    def sent(units, phase, step=1):
        for u in units:
            for src, dst, got, rank, tag in copies(u, phase, step):
                remote(src, dst, snd.at[u, tag], rcv.at[u, tag], rank).wait_send()

    cache, new = (0, 1), (2, 3)
    q_copy = remote(q_ref.at[pl.ds(4, 4)], qw.at[pl.ds(4, 4)], qsem.at[0], qsem.at[1], partner)
    start(cache, 1)
    q_copy.start()
    arrived(cache, 1)
    start(cache, 2, 1)
    start(new, 1)
    arrived(cache, 2, 1)
    start(cache, 2, 2)
    arrived(new, 1)
    start(new, 2, 1)
    arrived(cache, 2, 2)
    start(cache, 3, 0)
    start(cache, 3, 0.5)

    def event(at):
        @pl.when(at == 3)
        def _():
            q_copy.wait()
            arrived(new, 2, 1)
            start(new, 2, 2)

        @pl.when(at == 7)
        def _():
            arrived(cache, 3, 0)
            start(cache, 3, 3)

        @pl.when(at == 8)
        def _():
            arrived(new, 2, 2)
            start(new, 3, 0)
            start(new, 3, 0.5)

        @pl.when(at == 15)
        def _():
            arrived(cache, 3, 0.5)
            start(cache, 3, 4)

        @pl.when(at == 18)
        def _():
            arrived(new, 3, 0)
            start(new, 3, 3)

        @pl.when(at == 21)
        def _():
            arrived(new, 3, 0.5)
            start(new, 3, 4)

        @pl.when(at == 23)
        def _():
            arrived(cache, 3, 2)

        @pl.when(at == 27)
        def _():
            arrived(new, 3, 2)

    def cache_desc(chunk, prb):
        g, cg = div(chunk, 4), rem(chunk, 4)
        second = rem(cg, 2)
        near = (g == 1) | (g == 2)
        off = jnp.where(near, 1 + 2 * second, jnp.where(g == 0, 0, 2))
        half = jnp.where(near, g - 1, second)
        plane = rem(jnp.where(cg < 2, me["z"], me["x"]) + off, 4)
        base = plane * 16 + jnp.where(cg < 2, 0, 64) + half * 8
        return base, base + 4, prb

    def new_desc(c, prb):
        return 128 + rem(c, 4) * 16 + div(c, 4) * 4, 192 + 4 * c, prb

    def pick(cond, a, b):
        return tuple(lax.select(cond, i, j) for i, j in zip(a, b))

    def desc_first(b):
        c1 = cache_desc(4 * div(b, 8) + rem(b, 4), 4 * rem(div(b, 4), 2))
        c2 = cache_desc(12 + (b - 24), jnp.int32(4))
        c3 = new_desc(b - 28, jnp.int32(4))
        return pick(b < 24, c1, pick(b < 28, c2, c3))

    def desc_second(b):
        return pick(b < 4, cache_desc(12 + b, jnp.int32(0)), new_desc(b - 4, jnp.int32(0)))

    def desc_of(turn, b):
        return pick(turn == 0, desc_first(b), desc_second(b))

    def scores(d, u, i, mx):
        run4, j = buf.at[pl.ds(d[i // 2], 4)], 2 * (i % 2)
        kk = jnp.concatenate([run4[j, 0], run4[j + 1, 0]], axis=0)
        st = jnp.dot(kk, qw[d[2] + u], preferred_element_type=f32)
        s[i * 256:(i + 1) * 256, :] = st
        t = jnp.max(st.reshape(32, 8, WIDE), axis=0)
        return t if mx is None else jnp.maximum(mx, t)

    def step(d, dn, u, mx8):
        pr = d[2] + u
        nxt, un = (d, u + 1) if u + 1 < U else (dn, 0)
        mx = jnp.max(mx8, axis=0, keepdims=True) * SCALE2
        mo = m[pr]
        mn = jnp.maximum(mo, mx)
        alpha = jnp.exp2(mo - mn)
        m[pr] = mn
        ls = l[pr] * alpha
        weighted, mxn = None, None
        for i in range(SUBS):
            e = jnp.exp2(s[i * 256:(i + 1) * 256, :] * SCALE2 - mn)
            ls = ls + jnp.sum(e.reshape(32, 8, WIDE), axis=0)
            p[i % 2] = e.astype(bf16)
            mxn = scores(nxt, un, i, mxn)
            run4, j = buf.at[pl.ds(d[i // 2], 4)], 2 * (i % 2)
            vv = jnp.concatenate([run4[j, 1], run4[j + 1, 1]], axis=1)
            part = jnp.dot(vv, p[i % 2], preferred_element_type=f32)
            weighted = part if weighted is None else weighted + part
        l[pr] = ls
        acc[pr] = acc[pr] * alpha + weighted
        return mxn

    def masked_block(rank, prb, block):
        f = 128 + rem(div(block, 4), 4) * 16 + div(block, 16) * 4 + rem(block, 4)
        g = 192 + block
        key = block * ROWS + lax.broadcasted_iota(jnp.int32, (256, WIDE), 0)
        seen = key <= rank * ROWS + (lax.broadcasted_iota(jnp.int32, (256, WIDE), 1) & (ROWS - 1))
        kk = jnp.concatenate([buf[f, 0], buf[g, 0]], axis=0)
        vv = jnp.concatenate([buf[f, 1], buf[g, 1]], axis=1)
        for u in range(4):
            pr = prb + u
            st = jnp.where(seen, jnp.dot(kk, qw[pr], preferred_element_type=f32), MASK_VALUE)
            mx = jnp.max(jnp.max(st.reshape(32, 8, WIDE), axis=0), axis=0, keepdims=True) * SCALE2
            mo = m[pr]
            mn = jnp.maximum(mo, mx)
            alpha = jnp.exp2(mo - mn)
            m[pr] = mn
            e = jnp.exp2(st * SCALE2 - mn)
            l[pr] = l[pr] * alpha + jnp.sum(e.reshape(32, 8, WIDE), axis=0)
            acc[pr] = acc[pr] * alpha + jnp.dot(vv, e.astype(bf16), preferred_element_type=f32)

    o_copy = remote(osend, orecv, osem.at[0], osem.at[1], partner)

    def turn_body(turn, carry):
        rank = lax.select(turn == 0, partner, r)
        bodies = lax.select(turn == 0, jnp.int32(28), jnp.int32(4)) + div(rank, SUBS)
        prb = lax.select(turn == 0, jnp.int32(4), jnp.int32(0))
        d0 = desc_of(turn, jnp.int32(0))
        mx = None
        for i in range(SUBS):
            mx = scores(d0, 0, i, mx)

        def body(b, mx):
            event(b + 1000 * turn)
            d, dn = desc_of(turn, b), desc_of(turn, jnp.minimum(b + 1, bodies - 1))
            for u in range(U):
                mx = step(d, dn, u, mx)
            return mx

        lax.fori_loop(0, bodies, body, mx)
        start_block = rank - rem(rank, SUBS)

        def tail(j, carry):
            masked_block(rank, prb, start_block + j)
            return carry

        lax.fori_loop(0, rem(rank, SUBS) + 1, tail, 0)

        def result(h, carry):
            res = (acc[prb + h] / jnp.sum(l[prb + h], axis=0, keepdims=True)).T.astype(bf16)

            @pl.when(turn == 0)
            def _():
                osend[h] = res

            @pl.when(turn == 1)
            def _():
                out_ref[h] = res

            return carry

        lax.fori_loop(0, 4, result, 0)

        @pl.when(turn == 0)
        def _():
            o_copy.start()

        return carry

    lax.fori_loop(0, 2, turn_body, 0)
    o_copy.wait()
    out_ref[pl.ds(4, 4)] = orecv[...]

    for units in (cache, new):
        for phase, step in ((1, 1), (2, 1), (2, 2), (3, 0), (3, 0.5), (3, 2)):
            sent(units, phase, step)


def attend(q, own_cache, own_new):
    vm = pl.BlockSpec(memory_space=pltpu.VMEM)
    return pl.pallas_call(
        attn_kernel,
        out_shape=jax.ShapeDtypeStruct((8, WIDE, HEAD), bf16),
        in_specs=[vm] * 3,
        out_specs=vm,
        scratch_shapes=[
            pltpu.VMEM((256, 2, HALF, HEAD), bf16),
            pltpu.VMEM((8, HEAD, WIDE), bf16),
            pltpu.VMEM((8, HEAD, WIDE), f32),
            pltpu.VMEM((8, 1, WIDE), f32),
            pltpu.VMEM((8, 8, WIDE), f32),
            pltpu.VMEM((SUBS * 256, WIDE), f32),
            pltpu.VMEM((2, 256, WIDE), bf16),
            pltpu.VMEM((4, WIDE, HEAD), bf16),
            pltpu.VMEM((4, WIDE, HEAD), bf16),
            pltpu.SemaphoreType.DMA((4, 13)),
            pltpu.SemaphoreType.DMA((4, 13)),
            pltpu.SemaphoreType.DMA((4,)),
            pltpu.SemaphoreType.DMA((2,)),
            pltpu.SemaphoreType.DMA((2,)),
        ],
        compiler_params=pltpu.CompilerParams(collective_id=0, has_side_effects=True, vmem_limit_bytes=48 * 2 ** 20),
        name="attend",
    )(q, own_cache, own_new)


TILE = 512
TILES = 4096 // TILE


def out_kernel(o_ref, w_ref, x_ref, y_ref, o_s, mine, other, snd, rcv):
    step = pl.program_id(0)
    peer = 1 - lax.axis_index("tp")

    def copy(j):
        return pltpu.make_async_remote_copy(src_ref=mine.at[j], dst_ref=other.at[j], send_sem=snd.at[j], recv_sem=rcv.at[j],
                                            device_id={"tp": peer}, device_id_type=pl.DeviceIdType.MESH)

    @pl.when(step == 0)
    def _():
        barrier = pltpu.get_barrier_semaphore()
        pl.semaphore_signal(barrier, inc=1, device_id={"tp": peer}, device_id_type=pl.DeviceIdType.MESH)
        for h in range(HEADS):
            o_s[:, h * HEAD:(h + 1) * HEAD] = o_ref[h // 2, (h % 2) * ROWS:(h % 2 + 1) * ROWS, :]
        pl.semaphore_wait(barrier, 1)

    @pl.when(step < TILES)
    def _():
        mine[step] = jnp.dot(o_s[...], w_ref[...], preferred_element_type=f32)
        copy(step).start()

    @pl.when(step > 0)
    def _():
        copy(step - 1).wait()
        y_ref[...] = (x_ref[...].astype(f32) + (mine[step - 1] + other[step - 1])).astype(bf16)


def out_project(o, w_out, x):
    late = lambda j: (0, jnp.maximum(j - 1, 0))
    return pl.pallas_call(
        out_kernel,
        grid=(TILES + 1,),
        in_specs=[pl.BlockSpec((8, WIDE, HEAD), lambda j: (0, 0, 0)),
                  pl.BlockSpec((HEADS * HEAD, TILE), lambda j: (0, jnp.minimum(j, TILES - 1))),
                  pl.BlockSpec((ROWS, TILE), late)],
        out_specs=pl.BlockSpec((ROWS, TILE), late),
        out_shape=jax.ShapeDtypeStruct((ROWS, 4096), bf16),
        scratch_shapes=[pltpu.VMEM((ROWS, HEADS * HEAD), bf16), pltpu.VMEM((TILES, ROWS, TILE), f32),
                        pltpu.VMEM((TILES, ROWS, TILE), f32), pltpu.SemaphoreType.DMA((TILES,)), pltpu.SemaphoreType.DMA((TILES,))],
        compiler_params=pltpu.CompilerParams(collective_id=1, has_side_effects=True, vmem_limit_bytes=48 * 2 ** 20),
        name="outproj",
    )(o, w_out, x)


def local_step(x, k_cache, v_cache, rope_table, norm_gain, w_qkv, b_qkv, w_out):
    cos_t, sin_t = rope_table[:, :32], rope_table[:, 32:]
    cf = jnp.concatenate([jnp.repeat(cos_t, 2, axis=1), jnp.ones((ROWS, 64), f32)], axis=1)
    sf = jnp.concatenate([jnp.stack([-sin_t, sin_t], axis=-1).reshape(ROWS, 64), jnp.zeros((ROWS, 64), f32)], axis=1)
    q, new_k, new_v, own_new = project(x, norm_gain, cf, sf, w_qkv, b_qkv)
    kc = k_cache.reshape(2, HALF, HEAD)
    vc = v_cache.reshape(2, HALF, HEAD).transpose(0, 2, 1)
    own_cache = jnp.stack([kc, vc], axis=1)
    o = attend(q, own_cache, own_new)
    y = out_project(o, w_out, x)
    return y, new_k.reshape(ROWS, 1, HEAD), new_v.reshape(ROWS, 1, HEAD)


def solution(mesh):
    row_spec = P(('dp', 'cp'), None)
    cache_spec = P(('dp', 'cp'), 'tp', None)
    step = jax.shard_map(local_step, mesh=mesh, in_specs=(row_spec, cache_spec, cache_spec, row_spec, P(None), P(None, 'tp'), P('tp'), P('tp', None)), out_specs=(row_spec, cache_spec, cache_spec), check_vma=False)

    def run(*args):
        with jax.sharding.use_abstract_mesh(mesh.abstract_mesh):
            return step(*args)
    return run
```
